32 devices in a mesh: bank: 4 (over x, core), zero: 8 (over z, y).
Axes of the slice: x: 2, y: 2, z: 4, core: 2. Of those that a mesh axis runs over, the one named last changes fastest.
Arguments:
- w_gate: float32 [64, 2048, 1024], P('bank', 'zero'), may hold values from -0.1875 to 0.1875
- avg_gate: float32 [64, 2048, 1024], P('bank', 'zero'), may hold values from -0.125 to 0.125
- w_up: float32 [64, 2048, 1024], P('bank', 'zero'), may hold values from -0.1875 to 0.1875
- avg_up: float32 [64, 2048, 1024], P('bank', 'zero'), may hold values from -0.125 to 0.125
- mix_share: float32 [64], P('bank'), may hold values from 0.2 to 0.8
- router_weight: float32 [2048, 64], P('zero', 'bank'), may hold values from -0.125 to 0.125
- router_gain: float32 [2048], P('zero'), may hold values from 0.25 to 1.75
Outputs:
- serve_gate: bfloat16 [64, 2048, 1024], P('bank', None, 'zero')
- serve_up: bfloat16 [64, 2048, 1024], P('bank', None, 'zero')
- scale_gate: float32 [64, 1024], P('bank', 'zero')
- scale_up: float32 [64, 1024], P('bank', 'zero')
- serve_router: bfloat16 [2048, 64], replicated
The draws below stay inside these ranges and needn't reach their ends.
All inputs are finite; a program needn't handle non-finite values. Where the reference program divides by a largest or mean magnitude, that divisor is 1e-20 or more.
Results may differ from the reference program's by a relative error of at most 0.001.
Values may be sent and summed in bfloat16 or wider, within the bound.
A program may use at most 256 MiB of HBM per device.

```python
import jax
import jax.numpy as jnp

EXPERTS = 64
D_MODEL = 2048
D_EXPERT = 1024


def strengthened(drawn, key, source, target, parts, factor):
    def block_of(position):
        return (jnp.arange(drawn.shape[position]) // (drawn.shape[position] // parts)).reshape((-1,) + (1,) * (drawn.ndim - 1 - position))

    near = jax.random.permutation(key, parts)[block_of(target)]
    second = (block_of(target) + parts // 2) % parts
    return jnp.where((block_of(source) == near) | (block_of(source) == second), factor * drawn, drawn)


def levels(rng, dims, shards, smallest, largest):
    def one(axis_at, blocks):
        steps = jax.random.uniform(jax.random.fold_in(jax.random.fold_in(rng, 6), axis_at), (blocks,), jnp.float32, smallest / len(shards), largest / len(shards))
        return jnp.repeat(jnp.exp(steps), dims[axis_at] // blocks).reshape((-1,) + (1,) * (len(dims) - axis_at - 1))

    factor_of = one(*shards[0])
    for cut in shards[1:]:
        factor_of = factor_of * one(*cut)
    return factor_of


def gaussian(key, dims, deviation, most, pieces=(), kind=jnp.bfloat16):
    array = jax.random.normal(key, dims, jnp.float32) * deviation
    if len(pieces) > 0:
        array = levels(key, dims, pieces, -0.22, 0.18) * array
    return jnp.clip(array, min=-most, max=most).astype(kind)


def heavy_noise(stream_key, extent, scale, bound, pieces, heavy, held_as=jnp.bfloat16):
    array = scale * jax.random.normal(stream_key, extent, jnp.float32)
    if pieces:
        array = array * levels(stream_key, extent, pieces, -0.22, 0.18)
    return jnp.clip(strengthened(array, jax.random.fold_in(stream_key, 3), *heavy), -bound, bound).astype(held_as)


def setup_inputs(seed: int = 0) -> dict:
    arg_keys = jax.random.split(jax.random.key(seed), 8)
    w_gate = heavy_noise(arg_keys[0], (EXPERTS, D_MODEL, D_EXPERT), D_MODEL ** -0.5, 0.1875, ((0, 4), (1, 8)), (1, 2, 8, 2.0), jnp.float32)
    avg_gate = gaussian(arg_keys[1], (EXPERTS, D_MODEL, D_EXPERT), D_MODEL ** -0.5, 0.125, ((0, 4), (1, 8)), jnp.float32)
    w_up = heavy_noise(arg_keys[2], (EXPERTS, D_MODEL, D_EXPERT), D_MODEL ** -0.5, 0.1875, ((0, 4), (1, 8)), (1, 2, 8, 2.0), jnp.float32)
    avg_up = gaussian(arg_keys[3], (EXPERTS, D_MODEL, D_EXPERT), D_MODEL ** -0.5, 0.125, ((0, 4), (1, 8)), jnp.float32)
    mix_share = jnp.clip(0.2 + 0.6 * jax.random.uniform(arg_keys[4], (EXPERTS,), jnp.float32) ** levels(arg_keys[4], (EXPERTS,), ((0, 4),), -0.2, 0.2), 0.2, 0.8)
    router_weight = gaussian(arg_keys[5], (D_MODEL, EXPERTS), D_MODEL ** -0.5, 0.125, ((0, 8), (1, 4)), jnp.float32)
    router_gain = jnp.clip(1.0 + 0.15 * jax.random.normal(arg_keys[6], (D_MODEL,), jnp.float32), 0.25, 1.75)
    return {"w_gate": w_gate, "avg_gate": avg_gate, "w_up": w_up, "avg_up": avg_up, "mix_share": mix_share, "router_weight": router_weight, "router_gain": router_gain}


def reference(w_gate, avg_gate, w_up, avg_up, mix_share, router_weight, router_gain):
    fresh_gate = mix_share[:, None, None] * w_gate + (1.0 - mix_share[:, None, None]) * avg_gate
    fresh_up = mix_share[:, None, None] * w_up + (1.0 - mix_share[:, None, None]) * avg_up
    scale_gate = jnp.sum(jnp.abs(fresh_gate), axis=1) / D_MODEL
    serve_gate = (fresh_gate / jnp.expand_dims(scale_gate, 1)).astype(jnp.bfloat16)
    scale_up = jnp.sum(jnp.abs(fresh_up), axis=1) / D_MODEL
    serve_up = (fresh_up / jnp.expand_dims(scale_up, 1)).astype(jnp.bfloat16)
    serve_router = (router_weight * router_gain[:, None]).astype(jnp.bfloat16)
    return serve_gate, serve_up, scale_gate, scale_up, serve_router
```

```python
import functools

import jax
import jax.numpy as jnp
from jax import lax
from jax.experimental import pallas as pl
from jax.experimental.pallas import tpu as pltpu
from jax.sharding import PartitionSpec as P

MESH = pl.DeviceIdType.MESH
SLOTS = 4


def partner(me, k, n):
    out, bit = me, 1
    while bit < n:
        if k & bit:
            out = out + bit * (1 - 2 * ((me // bit) % 2))
        bit *= 2
    return out


def plan(experts):
    first = max(1, experts // 8)
    sizes = [first, first, experts - 2 * first]
    groups, at, row = [], 0, 0
    for i, size in enumerate(sizes):
        if i == 0:
            cuts = [size]
        elif i == 1:
            cuts = [size // 2, size - size // 2]
        else:
            step = max(1, size // 3)
            cuts = [step, step, size - 2 * step]
        pieces, p = [], at
        for c in cuts:
            if c > 0:
                pieces.append((p, c))
                p += c
        rows = -(-2 * size // 8) * 8
        groups.append((at, size, row, rows, pieces))
        at += size
        row += rows
    return groups, row


def kernel(
    nz, nb, groups,
    mix, wg, ag, wu, au, rw, gain,
    og, ou, sg, su, rt,
    fresh, stage, send, part, rs, scl, rtp,
    in_sem, bulk_ssem, bulk_rsem, own_sem, rs_ssem, rs_rsem, ag_ssem, ag_rsem,
    r1_ssem, r1_rsem, r2_ssem, r2_rsem, r_own,
):
    me = lax.axis_index("zero")
    bank = lax.axis_index("bank")
    experts, rows, _ = wg.shape
    cb = part.shape[2]
    eb = rw.shape[0]
    ws, avgs, outs, scales = (wg, wu), (ag, au), (og, ou), (sg, su)
    peers = [partner(me, k, nz) for k in range(1, nz)]
    banks = [partner(bank, k, nb) for k in range(1, nb)]

    def loads(e):
        slot = lax.rem(e, SLOTS)
        out = []
        for m in range(2):
            out.append(pltpu.make_async_copy(ws[m].at[e], fresh.at[m, e], in_sem.at[slot, m, 0]))
            out.append(pltpu.make_async_copy(avgs[m].at[e], stage.at[slot, m], in_sem.at[slot, m, 1]))
        return out

    for e in range(min(SLOTS, experts)):
        for c in loads(e):
            c.start()

    barrier = pltpu.get_barrier_semaphore()
    for p in peers:
        pl.semaphore_signal(barrier, inc=1, device_id={"zero": p}, device_id_type=MESH)
    for p in banks:
        pl.semaphore_signal(barrier, inc=1, device_id={"bank": p}, device_id_type=MESH)

    part[...] = jnp.zeros_like(part)
    rtp[...] = (rw[...] * gain[...]).astype(rtp.dtype)

    def compute(g):
        at, size, row0, _, _ = groups[g]

        def body(e, carry):
            slot = lax.rem(e, SLOTS)
            for c in loads(e):
                c.wait()
            a = mix[e]
            b = 1.0 - a
            for m in range(2):
                row = row0 + m * size + (e - at)
                for d in range(nz):
                    cols = slice(d * cb, (d + 1) * cb)
                    v = a * fresh[m, e, :, cols] + b * stage[slot, m, :, cols]
                    fresh[m, e, :, cols] = v
                    part[d, pl.ds(row, 1), :] = jnp.sum(jnp.abs(v), axis=0, keepdims=True)

            @pl.when(e + SLOTS < experts)
            def _():
                for c in loads(e + SLOTS):
                    c.start()

            return carry

        lax.fori_loop(at, at + size, body, 0)

    def scatter(g):
        _, _, row0, n, _ = groups[g]
        span = pl.ds(row0, n)
        out = []
        for k, p in enumerate(peers):
            out.append(pltpu.make_async_remote_copy(
                part.at[p, span], rs.at[k, span], rs_ssem.at[g, k], rs_rsem.at[g, k],
                device_id={"zero": p}, device_id_type=MESH))
            out[-1].start()
        return out

    def gather(g, pending):
        at, size, row0, n, _ = groups[g]
        span = pl.ds(row0, n)
        for c in pending:
            c.wait()
        total = part[me, span, :]
        for k in range(nz - 1):
            total = total + rs[k, span, :]
        total = total / (rows * nz)
        scl[me, span, :] = total
        for m in range(2):
            scales[m][at:at + size, :] = total[m * size:(m + 1) * size, :]
        out = []
        for k, p in enumerate(peers):
            out.append(pltpu.make_async_remote_copy(
                scl.at[me, span], scl.at[me, span], ag_ssem.at[g, k], ag_rsem.at[g, k],
                device_id={"zero": p}, device_id_type=MESH))
            out[-1].start()
        return out

    def narrow(g, lo, n):
        at, size, row0, _, _ = groups[g]

        def body(e, carry):
            for m in range(2):
                row = row0 + m * size + (e - at)
                for d in range(nz):
                    cols = slice(d * cb, (d + 1) * cb)
                    inverse = 1.0 / scl[d, pl.ds(row, 1), :]
                    send[m, d, e] = (fresh[m, e, :, cols] * inverse).astype(send.dtype)
            return carry

        lax.fori_loop(lo, lo + n, body, 0)

    place = pl.ds(pl.multiple_of(me * rows, rows), rows)
    flying = []
    count = [0]

    def push(lo, n):
        i = count[0]
        count[0] += 1
        span = pl.ds(lo, n)
        for k, p in enumerate(peers):
            for m in range(2):
                c = pltpu.make_async_remote_copy(
                    send.at[m, p, span], outs[m].at[span, place], bulk_ssem.at[i, m, k], bulk_rsem.at[i, m, k],
                    device_id={"zero": p}, device_id_type=MESH)
                c.start()
                flying.append(c)
        for m in range(2):
            c = pltpu.make_async_copy(send.at[m, me, span], outs[m].at[span, place], own_sem.at[i, m])
            c.start()
            flying.append(c)

    compute(0)
    pl.semaphore_wait(barrier, nz - 1 + nb - 1)
    rs0 = scatter(0)
    band = pl.ds(pl.multiple_of(bank * eb, eb), eb)
    if len(rt.shape) == 2:
        mine, column = rt.at[band, place], rt.at[band]
    else:
        mine, column = rt.at[me, band], rt.at[:, band]
    first = []
    for k, p in enumerate(peers):
        first.append(pltpu.make_async_remote_copy(
            rtp, mine, r1_ssem.at[k], r1_rsem.at[k], device_id={"zero": p}, device_id_type=MESH))
    first.append(pltpu.make_async_copy(rtp, mine, r_own))
    compute(1)
    rs1 = scatter(1)
    ag0 = gather(0, rs0)
    ag1 = gather(1, rs1)
    for c in first:
        c.start()
    for c in ag0:
        c.wait()
    for lo, n in groups[0][4]:
        narrow(0, lo, n)
        push(lo, n)
    compute(2)
    rs2 = scatter(2)
    for c in ag1:
        c.wait()
    pieces = groups[1][4]
    narrow(1, *pieces[0])
    push(*pieces[0])
    for lo, n in pieces[1:]:
        narrow(1, lo, n)
    for c in first:
        c.wait()
    for k, p in enumerate(banks):
        c = pltpu.make_async_remote_copy(
            column, column, r2_ssem.at[k], r2_rsem.at[k], device_id={"bank": p}, device_id_type=MESH)
        c.start()
        flying.append(c)
    ag2 = gather(2, rs2)
    for lo, n in pieces[1:]:
        push(lo, n)
    for c in ag2:
        c.wait()
    for lo, n in groups[2][4]:
        narrow(2, lo, n)
        push(lo, n)
    for c in flying:
        c.wait()


def solution(mesh):
    nz, nb = mesh.shape["zero"], mesh.shape["bank"]

    def on_device(w_gate, avg_gate, w_up, avg_up, mix_share, router_weight, router_gain):
        experts, rows, columns = w_gate.shape
        cb = columns // nz
        eb = router_weight.shape[1]
        groups, stat = plan(experts)
        npieces = sum(len(g[4]) for g in groups)
        anyspace = pl.BlockSpec(memory_space=pl.ANY)
        vmem = pl.BlockSpec(memory_space=pltpu.VMEM)
        dma = pltpu.SemaphoreType.DMA
        out = jax.ShapeDtypeStruct((experts, rows * nz, cb), jnp.bfloat16)
        scale = jax.ShapeDtypeStruct((experts, cb), jnp.float32)
        flat = rows % 128 == 0
        router = (eb * nb, rows * nz) if flat else (nz, eb * nb, rows)
        router = jax.ShapeDtypeStruct(router, jnp.bfloat16)
        ng = len(groups)
        sg, su, cg, cu, rt = pl.pallas_call(
            functools.partial(kernel, nz, nb, groups),
            out_shape=(out, out, scale, scale, router),
            in_specs=[pl.BlockSpec(memory_space=pltpu.SMEM)] + [anyspace] * 4 + [vmem] * 2,
            out_specs=(anyspace, anyspace, vmem, vmem, anyspace),
            scratch_shapes=[
                pltpu.VMEM((2, experts, rows, columns), jnp.float32),
                pltpu.VMEM((SLOTS, 2, rows, columns), jnp.float32),
                pltpu.VMEM((2, nz, experts, rows, cb), jnp.bfloat16),
                pltpu.VMEM((nz, stat, cb), jnp.float32),
                pltpu.VMEM((nz - 1, stat, cb), jnp.float32),
                pltpu.VMEM((nz, stat, cb), jnp.float32),
                pltpu.VMEM((eb, rows), jnp.bfloat16),
                dma((SLOTS, 2, 2)),
                dma((npieces, 2, nz - 1)),
                dma((npieces, 2, nz - 1)),
                dma((npieces, 2)),
                dma((ng, nz - 1)),
                dma((ng, nz - 1)),
                dma((ng, nz - 1)),
                dma((ng, nz - 1)),
                dma((nz - 1,)),
                dma((nz - 1,)),
                dma((nb - 1,)),
                dma((nb - 1,)),
                dma,
            ],
            compiler_params=pltpu.CompilerParams(
                collective_id=0, has_side_effects=True, vmem_limit_bytes=67_000_000
            ),
        )(mix_share, w_gate, avg_gate, w_up, avg_up, router_weight.T, router_gain[None, :])
        rt = rt.T if flat else rt.transpose(0, 2, 1).reshape(nz * rows, nb * eb)
        return sg, su, cg, cu, rt

    in_specs = (
        P("bank", "zero", None),
        P("bank", "zero", None),
        P("bank", "zero", None),
        P("bank", "zero", None),
        P("bank"),
        P("zero", "bank"),
        P("zero"),
    )
    out_specs = (
        P("bank", None, "zero"),
        P("bank", None, "zero"),
        P("bank", "zero"),
        P("bank", "zero"),
        P(),
    )
    return jax.shard_map(
        on_device, mesh=mesh, in_specs=in_specs, out_specs=out_specs, check_vma=False
    )
```

```python
import functools

import jax
import jax.numpy as jnp
from jax import lax
from jax.experimental import pallas as pl
from jax.experimental.pallas import tpu as pltpu
from jax.sharding import PartitionSpec as P

MESH = pl.DeviceIdType.MESH
SLOTS = 4


def partner(me, k, n):
    out, bit = me, 1
    while bit < n:
        if k & bit:
            out = out + bit * (1 - 2 * ((me // bit) % 2))
        bit *= 2
    return out


def plan(experts):
    first = max(1, experts // 16)
    sizes = [first, 3 * first, experts - 4 * first]
    groups, at, row = [], 0, 0
    for i, size in enumerate(sizes):
        if i == 0:
            cuts = [size]
        elif i == 1:
            cuts = [first] * 3
        else:
            step = max(1, size // 3)
            cuts = [step, step, size - 2 * step]
        pieces, p = [], at
        for c in cuts:
            if c > 0:
                pieces.append((p, c))
                p += c
        rows = -(-2 * size // 8) * 8
        groups.append((at, size, row, rows, pieces))
        at += size
        row += rows
    return groups, row


def kernel(
    nz, nb, groups,
    mix, wg, ag, wu, au, rw, gain,
    og, ou, sg, su, rt,
    fresh, stage, send, part, rs, scl, rtp,
    in_sem, bulk_ssem, bulk_rsem, own_sem, rs_ssem, rs_rsem, ag_ssem, ag_rsem,
    r1_ssem, r1_rsem, r2_ssem, r2_rsem, r_own,
):
    me = lax.axis_index("zero")
    bank = lax.axis_index("bank")
    experts, rows, _ = wg.shape
    cb = part.shape[2]
    eb = rw.shape[0]
    ws, avgs, outs, scales = (wg, wu), (ag, au), (og, ou), (sg, su)
    peers = [partner(me, k, nz) for k in range(1, nz)]
    banks = [partner(bank, k, nb) for k in range(1, nb)]

    def loads(e):
        slot = lax.rem(e, SLOTS)
        out = []
        for m in range(2):
            out.append(pltpu.make_async_copy(ws[m].at[e], fresh.at[m, e], in_sem.at[slot, m, 0]))
            out.append(pltpu.make_async_copy(avgs[m].at[e], stage.at[slot, m], in_sem.at[slot, m, 1]))
        return out

    for e in range(min(SLOTS, experts)):
        for c in loads(e):
            c.start()

    barrier = pltpu.get_barrier_semaphore()
    for p in peers:
        pl.semaphore_signal(barrier, inc=1, device_id={"zero": p}, device_id_type=MESH)
    for p in banks:
        pl.semaphore_signal(barrier, inc=1, device_id={"bank": p}, device_id_type=MESH)

    part[...] = jnp.zeros_like(part)
    rtp[...] = (rw[...] * gain[...]).astype(rtp.dtype)

    def compute(g):
        at, size, row0, _, _ = groups[g]

        def body(e, carry):
            slot = lax.rem(e, SLOTS)
            for c in loads(e):
                c.wait()
            a = mix[e]
            b = 1.0 - a
            for m in range(2):
                row = row0 + m * size + (e - at)
                for d in range(nz):
                    cols = slice(d * cb, (d + 1) * cb)
                    v = a * fresh[m, e, :, cols] + b * stage[slot, m, :, cols]
                    fresh[m, e, :, cols] = v
                    part[d, pl.ds(row, 1), :] = jnp.sum(jnp.abs(v), axis=0, keepdims=True)

            @pl.when(e + SLOTS < experts)
            def _():
                for c in loads(e + SLOTS):
                    c.start()

            return carry

        lax.fori_loop(at, at + size, body, 0)

    def scatter(g):
        _, _, row0, n, _ = groups[g]
        span = pl.ds(row0, n)
        out = []
        for k, p in enumerate(peers):
            out.append(pltpu.make_async_remote_copy(
                part.at[p, span], rs.at[k, span], rs_ssem.at[g, k], rs_rsem.at[g, k],
                device_id={"zero": p}, device_id_type=MESH))
            out[-1].start()
        return out

    def gather(g, pending):
        at, size, row0, n, _ = groups[g]
        span = pl.ds(row0, n)
        for c in pending:
            c.wait()
        total = part[me, span, :]
        for k in range(nz - 1):
            total = total + rs[k, span, :]
        total = total / (rows * nz)
        scl[me, span, :] = total
        for m in range(2):
            scales[m][at:at + size, :] = total[m * size:(m + 1) * size, :]
        out = []
        for k, p in enumerate(peers):
            out.append(pltpu.make_async_remote_copy(
                scl.at[me, span], scl.at[me, span], ag_ssem.at[g, k], ag_rsem.at[g, k],
                device_id={"zero": p}, device_id_type=MESH))
            out[-1].start()
        return out

    def narrow(g, lo, n):
        at, size, row0, _, _ = groups[g]

        def body(e, carry):
            for m in range(2):
                row = row0 + m * size + (e - at)
                for d in range(nz):
                    cols = slice(d * cb, (d + 1) * cb)
                    inverse = 1.0 / scl[d, pl.ds(row, 1), :]
                    send[m, d, e] = (fresh[m, e, :, cols] * inverse).astype(send.dtype)
            return carry

        lax.fori_loop(lo, lo + n, body, 0)

    place = pl.ds(pl.multiple_of(me * rows, rows), rows)
    flying = []
    count = [0]

    def push(lo, n):
        i = count[0]
        count[0] += 1
        span = pl.ds(lo, n)
        for k, p in enumerate(peers):
            for m in range(2):
                c = pltpu.make_async_remote_copy(
                    send.at[m, p, span], outs[m].at[span, place], bulk_ssem.at[i, m, k], bulk_rsem.at[i, m, k],
                    device_id={"zero": p}, device_id_type=MESH)
                c.start()
                flying.append(c)
        for m in range(2):
            c = pltpu.make_async_copy(send.at[m, me, span], outs[m].at[span, place], own_sem.at[i, m])
            c.start()
            flying.append(c)

    compute(0)
    pl.semaphore_wait(barrier, nz - 1 + nb - 1)
    rs0 = scatter(0)
    band = pl.ds(pl.multiple_of(bank * eb, eb), eb)
    if len(rt.shape) == 2:
        mine, column = rt.at[band, place], rt.at[band]
    else:
        mine, column = rt.at[me, band], rt.at[:, band]
    first = []
    for k, p in enumerate(peers):
        first.append(pltpu.make_async_remote_copy(
            rtp, mine, r1_ssem.at[k], r1_rsem.at[k], device_id={"zero": p}, device_id_type=MESH))
    first.append(pltpu.make_async_copy(rtp, mine, r_own))
    compute(1)
    rs1 = scatter(1)
    ag0 = gather(0, rs0)
    ag1 = gather(1, rs1)
    for c in first:
        c.start()
    for c in ag0:
        c.wait()
    for lo, n in groups[0][4]:
        narrow(0, lo, n)
        push(lo, n)
    for c in ag1:
        c.wait()
    early, middle, late = groups[1][4]
    narrow(1, *early)
    push(*early)
    compute(2)
    rs2 = scatter(2)
    narrow(1, *middle)
    push(*middle)
    narrow(1, *late)
    for c in first:
        c.wait()
    for k, p in enumerate(banks):
        c = pltpu.make_async_remote_copy(
            column, column, r2_ssem.at[k], r2_rsem.at[k], device_id={"bank": p}, device_id_type=MESH)
        c.start()
        flying.append(c)
    ag2 = gather(2, rs2)
    push(*late)
    for c in ag2:
        c.wait()
    for lo, n in groups[2][4]:
        narrow(2, lo, n)
        push(lo, n)
    for c in flying:
        c.wait()


def settle(count, *refs):
    sources, targets, buffers = refs[:count], refs[count:2 * count], refs[2 * count:3 * count]
    big_in, big_out, small_in, small_out = refs[3 * count:]
    jobs = []
    for i in range(2):
        for e in range(sources[i].shape[0]):
            jobs.append((sources[i].at[e], buffers[i].at[e], targets[i].at[e], big_in.at[i, e], big_out.at[i, e]))
    for i in range(2, count):
        jobs.append((sources[i], buffers[i], targets[i], small_in.at[i - 2], small_out.at[i - 2]))
    reads = [pltpu.make_async_copy(src, buf, sem) for src, buf, _, sem, _ in jobs]
    writes = [pltpu.make_async_copy(buf, dst, sem) for _, buf, dst, _, sem in jobs]
    for r in reads:
        r.start()
    for r, w in zip(reads, writes):
        r.wait()
        w.start()
    for w in writes:
        w.wait()


def solution(mesh):
    nz, nb = mesh.shape["zero"], mesh.shape["bank"]

    def on_device(w_gate, avg_gate, w_up, avg_up, mix_share, router_weight, router_gain):
        experts, rows, columns = w_gate.shape
        cb = columns // nz
        eb = router_weight.shape[1]
        groups, stat = plan(experts)
        npieces = sum(len(g[4]) for g in groups)
        anyspace = pl.BlockSpec(memory_space=pl.ANY)
        vmem = pl.BlockSpec(memory_space=pltpu.VMEM)
        dma = pltpu.SemaphoreType.DMA
        out = jax.ShapeDtypeStruct((experts, rows * nz, cb), jnp.bfloat16)
        scale = jax.ShapeDtypeStruct((experts, cb), jnp.float32)
        flat = rows % 128 == 0
        router = (eb * nb, rows * nz) if flat else (nz, eb * nb, rows)
        router = jax.ShapeDtypeStruct(router, jnp.bfloat16)
        ng = len(groups)
        landed = pl.pallas_call(
            functools.partial(kernel, nz, nb, groups),
            out_shape=(out, out, scale, scale, router),
            in_specs=[pl.BlockSpec(memory_space=pltpu.SMEM)] + [anyspace] * 4 + [vmem] * 2,
            out_specs=(anyspace, anyspace, vmem, vmem, anyspace),
            scratch_shapes=[
                pltpu.VMEM((2, experts, rows, columns), jnp.float32),
                pltpu.VMEM((SLOTS, 2, rows, columns), jnp.float32),
                pltpu.VMEM((2, nz, experts, rows, cb), jnp.bfloat16),
                pltpu.VMEM((nz, stat, cb), jnp.float32),
                pltpu.VMEM((nz - 1, stat, cb), jnp.float32),
                pltpu.VMEM((nz, stat, cb), jnp.float32),
                pltpu.VMEM((eb, rows), jnp.bfloat16),
                dma((SLOTS, 2, 2)),
                dma((npieces, 2, nz - 1)),
                dma((npieces, 2, nz - 1)),
                dma((npieces, 2)),
                dma((ng, nz - 1)),
                dma((ng, nz - 1)),
                dma((ng, nz - 1)),
                dma((ng, nz - 1)),
                dma((nz - 1,)),
                dma((nz - 1,)),
                dma((nb - 1,)),
                dma((nb - 1,)),
                dma,
            ],
            compiler_params=pltpu.CompilerParams(
                collective_id=0, has_side_effects=True, vmem_limit_bytes=67_000_000
            ),
        )(mix_share, w_gate, avg_gate, w_up, avg_up, router_weight.T, router_gain[None, :])
        shapes = (out, out, scale, scale, router)
        sg, su, cg, cu, rt = pl.pallas_call(
            functools.partial(settle, len(shapes)),
            out_shape=shapes,
            in_specs=[anyspace] * len(shapes),
            out_specs=(anyspace,) * len(shapes),
            scratch_shapes=[pltpu.VMEM(x.shape, x.dtype) for x in shapes]
            + [dma((2, experts))] * 2
            + [dma((len(shapes) - 2,))] * 2,
            compiler_params=pltpu.CompilerParams(vmem_limit_bytes=60_000_000),
        )(*landed)
        rt = rt.T if flat else rt.transpose(0, 2, 1).reshape(nz * rows, nb * eb)
        return sg, su, cg, cu, rt

    in_specs = (
        P("bank", "zero", None),
        P("bank", "zero", None),
        P("bank", "zero", None),
        P("bank", "zero", None),
        P("bank"),
        P("zero", "bank"),
        P("zero"),
    )
    out_specs = (
        P("bank", None, "zero"),
        P("bank", None, "zero"),
        P("bank", "zero"),
        P("bank", "zero"),
        P(),
    )
    return jax.shard_map(
        on_device, mesh=mesh, in_specs=in_specs, out_specs=out_specs, check_vma=False
    )
```
